32 devices in a mesh: scan: 16 (over z, x, core), tile: 2 (over y).
Axes of the slice: x: 2, y: 2, z: 4, core: 2. Of those that a mesh axis runs over, the one named last changes fastest.
Arguments:
- probe_modes: float32 [12, 2, 128, 128], replicated, may hold values from -5 to 5
- patterns: float32 [128, 128, 128], P(('scan', 'tile')), may hold values from 0.005 to 300
- specimen: float32 [2, 2048, 512], P(None, 'scan', 'tile'), may hold values from -17.5 to 17.5
- offsets: int32 [128, 2], P(('scan', 'tile')), may hold values from -128 to 2048, as said below
Outputs:
- new_probe: float32 [12, 2, 128, 128], replicated
- new_specimen: float32 [2, 2048, 512], P(None, 'scan', 'tile')
The draws below stay inside these ranges and needn't reach their ends.
Inputs may be any that keep to these rules, and one draw needn't show every extreme that they name: `offsets`: position p lies in aligned block b = p // 4, held by the device of scan index s = b // (the number of tile devices) and tile index t = b % (the number of tile devices); its row offset lies in s * 128 - 128 to s * 128 + 128, its column offset in t * 256 - 128 to t * 256 + 256, both ends included; in every block one position has its row offset at the lower end and its column offset at the upper end, and one has its row offset at the upper end.
All inputs are finite; a program needn't handle non-finite values.
Results may differ from the reference program's by a relative error of at most 0.0001.
Values sent between devices are 32-bit elements; how exact they have to be, the bound alone decides.
No kernel may reach another device: no remote copies, remote signals or barrier semaphores. Data moves between devices by JAX's collectives and lax.ppermute only.
A program may use at most 64 MiB of HBM per device.

```python
import math
import jax
import jax.numpy as jnp
from jax import lax

DET = 128
MODES = 12
P_DEV = 4
ROWS_DEV = 128
COLS_DEV = 256
NS_STEPS = 8
POSITIONS = 128
OBJ_ROWS = 2048
OBJ_COLS = 512


def draw_probe_modes(key, part):
    key_base, key_weight = jax.random.split(key, 2)
    shape_all = (MODES, 2, DET, DET)
    base_field = jnp.clip(jax.random.normal(key_base, shape_all, jnp.float32), -5.0, 5.0)
    weights = jnp.exp(jax.random.uniform(key_weight, (MODES,), jnp.float32, math.log(0.1), math.log(0.4)))
    mixing = 0.6
    weights = weights.at[0].set(1.0)
    mixed = base_field + mixing * base_field[0:1]
    mixed = mixed.at[0].set(base_field[0])
    return (mixed * weights[:, None, None, None]).astype(jnp.float32)


def draw_patterns(key, part):
    key_flux, key_pixel, key_speckle = jax.random.split(key, 3)
    block_count = POSITIONS // P_DEV
    along = (jnp.arange(POSITIONS, dtype=jnp.int32) // P_DEV).astype(jnp.float32) / max(block_count - 1, 1)
    flux_low, flux_high, growth, speck_low, speck_high = (1.0, 6.0, 3.0, 0.2, 1.8)
    flux = jnp.exp(jax.random.uniform(key_flux, (POSITIONS,), jnp.float32, math.log(flux_low), math.log(flux_high))) * growth ** along
    pixel_gain = jnp.exp(jax.random.uniform(key_pixel, (DET, DET), jnp.float32, math.log(0.3), math.log(3.0)))
    speckle = jax.random.uniform(key_speckle, (POSITIONS, DET, DET), jnp.float32, speck_low, speck_high)
    return (flux[:, None, None] * pixel_gain[None] * speckle).astype(jnp.float32)


def draw_specimen(key, part):
    key_values, key_rows, key_cols = jax.random.split(key, 3)
    values = 0.4 * jnp.clip(jax.random.normal(key_values, (2, OBJ_ROWS, OBJ_COLS), jnp.float32), -4.0, 4.0)
    mean_part = 1.0
    row_scale = jnp.exp(jax.random.uniform(key_rows, (OBJ_ROWS,), jnp.float32, math.log(0.5), math.log(2.0)))
    col_scale = jnp.exp(jax.random.uniform(key_cols, (OBJ_COLS,), jnp.float32, math.log(0.5), math.log(2.0)))
    rough = values * row_scale[None, :, None] * col_scale[None, None, :]
    shift = jnp.array([mean_part, 0.0], jnp.float32)[:, None, None]
    return (rough + shift).astype(jnp.float32)


def draw_offsets(key, part):
    key_rows, key_cols = jax.random.split(key, 2)
    tile_count = OBJ_COLS // COLS_DEV
    position = jnp.arange(POSITIONS, dtype=jnp.int32)
    group_index = position // P_DEV
    within = position % P_DEV
    scan_index = group_index // tile_count
    tile_index = group_index % tile_count
    local_row = jax.random.randint(key_rows, (POSITIONS,), 0, ROWS_DEV + DET + 1, dtype=jnp.int32)
    local_col = jax.random.randint(key_cols, (POSITIONS,), 0, COLS_DEV + DET + 1, dtype=jnp.int32)
    local_row = jnp.where(within == 0, 0, jnp.where(within == 1, ROWS_DEV + DET, local_row))
    local_col = jnp.where(within == 0, COLS_DEV + DET, local_col)
    row_offsets = scan_index * ROWS_DEV - DET + local_row
    col_offsets = tile_index * COLS_DEV - DET + local_col
    return jnp.stack([row_offsets, col_offsets], axis=1).astype(jnp.int32)


def setup_inputs(seed: int = 0) -> dict:
    splits = jax.random.split(jax.random.key(seed), 5)
    return {
        "probe_modes": draw_probe_modes(jax.random.fold_in(splits[4], 71), 0),
        "patterns": draw_patterns(jax.random.fold_in(splits[4], 71), 0),
        "specimen": draw_specimen(jax.random.fold_in(splits[4], 71), 0),
        "offsets": draw_offsets(jax.random.fold_in(splits[4], 71), 0),
    }


highest = lax.Precision.HIGHEST
light_floor = 0.05
object_reg = 0.5
probe_reg = 1.0
total_eps = 1e-06

def newton_steps(gram_re, gram_im):
    mode_count = gram_re.shape[0]
    upper = jnp.concatenate([gram_re, -gram_im], axis=1)
    lower = jnp.concatenate([gram_im, gram_re], axis=1)
    embedded = jnp.concatenate([upper, lower], axis=0)
    frobenius = jnp.sqrt(jnp.sum(embedded * embedded))
    identity = jnp.eye(2 * mode_count, dtype=jnp.float32)
    current = embedded / frobenius
    inverse = identity
    for repeat in range(NS_STEPS):
        factor = 1.5 * identity - 0.5 * jnp.dot(inverse, current, precision=highest, preferred_element_type=jnp.float32)
        current = jnp.dot(current, factor, precision=highest, preferred_element_type=jnp.float32)
        inverse = jnp.dot(factor, inverse, precision=highest, preferred_element_type=jnp.float32)
    inverse = inverse / jnp.sqrt(frobenius)
    return (inverse[:mode_count, :mode_count], inverse[mode_count:, :mode_count])

def gram_parts(mode_rows):
    real_rows = mode_rows[0::2]
    imag_rows = mode_rows[1::2]
    gram_re = jnp.dot(real_rows, real_rows.T, precision=highest, preferred_element_type=jnp.float32) + jnp.dot(imag_rows, imag_rows.T, precision=highest, preferred_element_type=jnp.float32)
    gram_im = jnp.dot(real_rows, imag_rows.T, precision=highest, preferred_element_type=jnp.float32) - jnp.dot(imag_rows, real_rows.T, precision=highest, preferred_element_type=jnp.float32)
    return (gram_re, gram_im)

def orthonormal_rows(mode_rows, gram_re, gram_im, power_ratio):
    real_rows = mode_rows[0::2]
    imag_rows = mode_rows[1::2]
    mix_re, mix_im = newton_steps(gram_re, gram_im)
    ortho_re = jnp.dot(mix_re.T, real_rows, precision=highest, preferred_element_type=jnp.float32) - jnp.dot(mix_im.T, imag_rows, precision=highest, preferred_element_type=jnp.float32)
    ortho_im = jnp.dot(mix_im.T, real_rows, precision=highest, preferred_element_type=jnp.float32) + jnp.dot(mix_re.T, imag_rows, precision=highest, preferred_element_type=jnp.float32)
    weight = jnp.sqrt(power_ratio * jnp.diagonal(gram_re))
    joined = jnp.stack([ortho_re, ortho_im], axis=1) * weight[:, None, None]
    return joined.reshape(mode_rows.shape)

def reference(probe_modes, patterns, specimen, offsets):
    detector = probe_modes.shape[-1]
    mode_count = probe_modes.shape[0]
    probe_field = lax.complex(probe_modes[:, 0], probe_modes[:, 1])
    probe_power = lax.optimization_barrier(jnp.sum(probe_modes[:, 0] ** 2 + probe_modes[:, 1] ** 2, axis=0))
    padded = jnp.pad(lax.complex(specimen[0], specimen[1]), ((detector, detector), (detector, detector)))
    frame_zeros = jnp.zeros(padded.shape, jnp.float32)
    mode_zeros = jnp.zeros((mode_count, detector, detector), jnp.float32)

    def one_position(position, running):
        grad_sum, light_sum, frame_num, frame_light, model_sum = running
        row_at = (offsets[position, 0] + detector).astype(jnp.int32)
        col_at = (offsets[position, 1] + detector).astype(jnp.int32)
        patch_now = lax.dynamic_slice(padded, (row_at, col_at), (detector, detector))
        exit_wave = probe_field * patch_now[None]
        model_sum = model_sum + jnp.sum(jnp.real(exit_wave) ** 2 + jnp.imag(exit_wave) ** 2)
        far_field = jnp.fft.fft2(exit_wave, norm='ortho')
        model_light = lax.optimization_barrier(jnp.sum(jnp.real(far_field) ** 2 + jnp.imag(far_field) ** 2, axis=0))
        factor = jnp.sqrt(patterns[position]) / jnp.sqrt(jnp.maximum(model_light, light_floor)) - 1.0
        change = jnp.fft.ifft2(far_field * factor[None], norm='ortho')
        grad_sum = grad_sum + jnp.conj(patch_now)[None] * change
        light_sum = light_sum + jnp.real(patch_now) ** 2 + jnp.imag(patch_now) ** 2
        contribution = lax.optimization_barrier(jnp.sum(jnp.conj(probe_field) * change, axis=0))
        old_num = lax.dynamic_slice(frame_num, (row_at, col_at), (detector, detector))
        frame_num = lax.dynamic_update_slice(frame_num, old_num + contribution, (row_at, col_at))
        old_light = lax.dynamic_slice(frame_light, (row_at, col_at), (detector, detector))
        frame_light = lax.dynamic_update_slice(frame_light, old_light + probe_power, (row_at, col_at))
        return (grad_sum, light_sum, frame_num, frame_light, model_sum)
    initial = (lax.complex(mode_zeros, mode_zeros), jnp.zeros((detector, detector), jnp.float32), lax.complex(frame_zeros, frame_zeros), frame_zeros, jnp.zeros((), jnp.float32))
    grad_sum, light_sum, frame_num, frame_light, model_sum = lax.fori_loop(0, POSITIONS, one_position, initial)
    interior_num = frame_num[detector:-detector, detector:-detector]
    interior_light = frame_light[detector:-detector, detector:-detector]
    new_field = padded[detector:-detector, detector:-detector] + interior_num / (interior_light + object_reg)
    new_specimen = jnp.stack([jnp.real(new_field), jnp.imag(new_field)])
    updated = probe_field + grad_sum / (light_sum + probe_reg)[None]
    updated_rows = jnp.stack([jnp.real(updated), jnp.imag(updated)], axis=1).reshape(2 * mode_count, -1)
    power_ratio = jnp.sum(patterns) / (model_sum + total_eps)
    gram_re, gram_im = gram_parts(updated_rows)
    new_rows = orthonormal_rows(updated_rows, gram_re, gram_im, power_ratio)
    return (new_rows.reshape(probe_modes.shape), new_specimen)
```

```python
import math

import jax
import jax.numpy as jnp
import numpy as np
from jax import lax
from jax.experimental import pallas as pl
from jax.experimental.pallas import tpu as pltpu
from jax.sharding import PartitionSpec as P

NS_STEPS = 8
AXES = ("scan", "tile")
light_floor = 0.05
object_reg = 0.5
probe_reg = 1.0
total_eps = 1e-06
f32 = jnp.float32
bf16 = jnp.bfloat16
highest = lax.Precision.HIGHEST


def dft_tables(detector):
    index = np.arange(detector, dtype=np.int64)
    angle = -2.0 * np.pi / detector * (index[:, None] * index[None, :] % detector)
    cos = np.cos(angle) / math.sqrt(detector)
    sin = np.sin(angle) / math.sqrt(detector)
    first = np.block([[cos, sin], [-sin, cos]]).astype(np.float32)
    second = np.block([[cos, -sin], [sin, cos]]).astype(np.float32)
    tables = []
    for table in (first, second):
        high = table.astype(bf16)
        low = (table - high.astype(np.float32)).astype(bf16)
        tables.append((high, low))
    (fh, fl), (sh, sl) = tables
    right_fwd = np.concatenate([fh, fh, fl], axis=0)
    right_inv = np.concatenate([sh, sh, sl], axis=0)
    left_fwd = np.concatenate([sh, sh, sl], axis=1)
    left_inv = np.concatenate([fh, fh, fl], axis=1)
    return tuple(jnp.asarray(t) for t in (right_fwd, left_fwd, right_inv, left_inv))


def split(values):
    high = values.astype(bf16)
    low = (values - high.astype(f32)).astype(bf16)
    return high, low


def right_product(rows, table):
    high, low = split(rows)
    return jnp.dot(jnp.concatenate([high, low, high], axis=1), table, preferred_element_type=f32)


def left_product(table, columns):
    high, low = split(columns)
    return jnp.dot(table, jnp.concatenate([high, low, high], axis=0), preferred_element_type=f32)


def to_columns(rows, n):
    top = jnp.concatenate([rows[:n, :n], rows[n:, :n]], axis=1)
    bottom = jnp.concatenate([rows[:n, n:], rows[n:, n:]], axis=1)
    return jnp.concatenate([top, bottom], axis=0)


def positions_kernel(
    where, probe, patterns, own, side_a, side_b, strip_y, strip_a, strip_b,
    right_fwd, left_fwd, right_inv, left_inv,
    sums, fold_own, fold_a, fold_b, fold_y, fold_ya, fold_yb,
    extended, frame, far, patch, model, power, numer,
):
    modes, _, n, _ = probe.shape
    count = patterns.shape[0]
    rows, cols = own.shape[1:]
    even = where[2 * count] == 0
    first_tile = where[2 * count + 1] == 0
    row_a = pl.multiple_of(jnp.where(even, n + rows, 0), n)
    row_b = pl.multiple_of(jnp.where(even, 0, n + rows), n)
    col_y = pl.multiple_of(jnp.where(first_tile, n + cols, 0), n)
    col_z = pl.multiple_of(jnp.where(first_tile, 0, n + cols), n)

    frame[...] = jnp.zeros_like(frame)
    extended[:, :, pl.ds(col_z, n)] = jnp.zeros((2, extended.shape[1], n), f32)
    extended[:, n : n + rows, n : n + cols] = own[...]
    extended[:, pl.ds(row_a, n), n : n + cols] = side_a[...]
    extended[:, pl.ds(row_b, n), n : n + cols] = side_b[...]
    extended[:, n : n + rows, pl.ds(col_y, n)] = strip_y[...]
    extended[:, pl.ds(row_a, n), pl.ds(col_y, n)] = strip_a[...]
    extended[:, pl.ds(row_b, n), pl.ds(col_y, n)] = strip_b[...]

    total = jnp.zeros((n, n), f32)
    for k in range(modes):
        total = total + probe[k, 0] * probe[k, 0] + probe[k, 1] * probe[k, 1]
    power[...] = total
    sums[...] = jnp.zeros_like(sums)
    pairs = modes // 2

    def one_position(p, carry):
        row = where[p]
        col = where[count + p]
        col_block = pl.multiple_of(col // n * n, n)
        shift = col - col_block
        row_block = pl.multiple_of(row // 8 * 8, 8)
        down = row - row_block
        for c in range(2):
            window = extended[c, pl.ds(row_block, n + 8), pl.ds(col_block, 2 * n)]
            window = pltpu.roll(window, (2 * n - shift) % (2 * n), 1)[:, :n]
            patch[c] = pltpu.roll(window, (n + 8 - down) % (n + 8), 0)[:n]
        model[...] = jnp.zeros_like(model)

        def forward(q, carry):
            p_re = patch[0]
            p_im = patch[1]
            blocks = []
            for k in range(2):
                re = probe[2 * q + k, 0]
                im = probe[2 * q + k, 1]
                blocks.append(
                    jnp.concatenate([re * p_re - im * p_im, re * p_im + im * p_re], axis=1)
                )
            half = right_product(jnp.concatenate(blocks, axis=0), right_fwd[...])
            full = left_product(left_fwd[...], to_columns(half, n))
            far[q] = full
            squares = full * full
            squares = squares[:n] + squares[n:]
            model[...] += squares[:, :n] + squares[:, n:]
            return carry

        lax.fori_loop(0, pairs, forward, 0, unroll=UNROLL)
        light = model[...]
        measured = patterns[p]
        factor = jnp.sqrt(measured) / jnp.sqrt(jnp.maximum(light, light_floor)) - 1.0
        model[...] = factor
        sums[2 * modes + 1, 0:8] += jnp.sum(light.reshape(n // 8, 8, n), axis=0)
        sums[2 * modes + 1, 8:16] += jnp.sum(measured.reshape(n // 8, 8, n), axis=0)
        numer[...] = jnp.zeros_like(numer)

        def backward(q, carry):
            factor = model[...]
            factor4 = jnp.concatenate([factor, factor], axis=1)
            factor4 = jnp.concatenate([factor4, factor4], axis=0)
            half = right_product(to_columns(far[q] * factor4, n), right_inv[...])
            change = left_product(left_inv[...], to_columns(half, n))
            p_re = patch[0]
            p_im = patch[1]
            num_re = numer[0]
            num_im = numer[1]
            for k in range(2):
                c_re = change[:n, k * n : (k + 1) * n]
                c_im = change[n:, k * n : (k + 1) * n]
                re = probe[2 * q + k, 0]
                im = probe[2 * q + k, 1]
                at = 4 * q + 2 * k
                sums[at] += p_re * c_re + p_im * c_im
                sums[at + 1] += p_re * c_im - p_im * c_re
                num_re = num_re + (re * c_re + im * c_im)
                num_im = num_im + (re * c_im - im * c_re)
            numer[0] = num_re
            numer[1] = num_im
            return carry

        lax.fori_loop(0, pairs, backward, 0, unroll=UNROLL)
        sums[2 * modes] += patch[0] * patch[0] + patch[1] * patch[1]
        for c in range(3):
            value = power[...] if c == 2 else numer[c]
            tall = pltpu.roll(jnp.concatenate([value, jnp.zeros((8, n), f32)], axis=0), down, 0)
            wide = pltpu.roll(jnp.concatenate([tall, jnp.zeros_like(tall)], axis=1), shift, 1)
            frame[c, pl.ds(row_block, n + 8), pl.ds(col_block, 2 * n)] += wide
        return carry

    lax.fori_loop(0, count, one_position, 0)
    fold_own[...] = frame[:, n : n + rows, n : n + cols]
    fold_a[...] = frame[:, pl.ds(row_a, n), n : n + cols]
    fold_b[...] = frame[:, pl.ds(row_b, n), n : n + cols]
    fold_y[...] = frame[:, n : n + rows, pl.ds(col_y, n)]
    fold_ya[...] = frame[:, pl.ds(row_a, n), pl.ds(col_y, n)]
    fold_yb[...] = frame[:, pl.ds(row_b, n), pl.ds(col_y, n)]


UNROLL = 2


def object_kernel(where, specimen, own, side_a, side_b, strip_y, strip_a, strip_b, out):
    n = strip_y.shape[2]
    cols = own.shape[2]
    first_tile = where[where.shape[0] - 1] == 0
    at = pl.multiple_of(jnp.where(first_tile, cols - n, 0), n)
    own[...] += side_a[...] + side_b[...]
    own[:, :, pl.ds(at, n)] += strip_y[...] + strip_a[...] + strip_b[...]
    light = own[2] + object_reg
    out[0] = specimen[0] + own[0] / light
    out[1] = specimen[1] + own[1] / light


def probe_kernel(*refs):
    probe = refs[0]
    pieces = refs[1:-2]
    out, updated = refs[-2:]
    modes, _, n, _ = probe.shape
    rows = pieces[0].shape[0]
    per = n // rows
    planes = 2 * modes
    for part in range(per):
        at = slice(part * rows, (part + 1) * rows)
        light = pieces[planes * per + part][...] + probe_reg
        for k in range(planes):
            updated[k, at] = probe[k // 2, k % 2, at] + pieces[k * per + part][...] / light
    tail = pieces[(planes + 1) * per]
    model_all = jnp.sum(tail[0:8, :], keepdims=True)
    measured_all = jnp.sum(tail[8:16, :], keepdims=True)
    ratio = measured_all / (model_all + total_eps)
    step = 16
    gram = jnp.zeros((planes, planes), f32)
    for x in range(0, n, step):
        chunk = jnp.concatenate([updated[:, x + i, :] for i in range(step)], axis=1)
        gram = gram + lax.dot_general(
            chunk, chunk, (((1,), (1,)), ((), ())), precision=highest, preferred_element_type=f32
        )
    i0 = lax.broadcasted_iota(jnp.int32, (planes, planes), 0)
    i1 = lax.broadcasted_iota(jnp.int32, (planes, planes), 1)
    identity = jnp.where(i0 == i1, 1.0, 0.0)
    turn = jnp.where(i0 == i1 + 1, jnp.where(i1 % 2 == 0, 1.0, 0.0), 0.0) - jnp.where(
        i1 == i0 + 1, jnp.where(i0 % 2 == 0, 1.0, 0.0), 0.0
    )

    def mul(a, b):
        return jnp.dot(a, b, precision=highest, preferred_element_type=f32)

    hermitian = gram - mul(mul(turn, gram), turn)
    frobenius = jnp.sqrt(jnp.sum(hermitian * hermitian, keepdims=True))
    current = hermitian / frobenius
    inverse = identity
    for _ in range(NS_STEPS):
        factor = 1.5 * identity - 0.5 * mul(inverse, current)
        current = mul(current, factor)
        inverse = mul(factor, inverse)
    inverse = inverse / jnp.sqrt(frobenius)
    diagonal = jnp.sum(hermitian * identity, axis=1, keepdims=True)
    mix = inverse * jnp.sqrt(ratio * diagonal)
    for x in range(0, n, step):
        chunk = jnp.concatenate([updated[:, x + i, :] for i in range(step)], axis=1)
        mixed = mul(mix, chunk)
        for i in range(step):
            out[:, x + i, :] = mixed[:, i * n : (i + 1) * n]


def vmem(count):
    return [pl.BlockSpec(memory_space=pltpu.VMEM)] * count


def partners(scan, tile):
    def flat(s, t):
        return s * tile + t

    mates, others, across, mates_across, others_across = [], [], [], [], []
    for s in range(scan):
        mate = s ^ 1
        other = s + 1 if s % 2 else s - 1
        for t in range(tile):
            here = flat(s, t)
            mates.append((here, flat(mate, t)))
            across.append((here, flat(s, 1 - t)))
            mates_across.append((here, flat(mate, 1 - t)))
            if 0 <= other < scan:
                others.append((here, flat(other, t)))
                others_across.append((here, flat(other, 1 - t)))
    return mates, others, across, mates_across, others_across


def body(probe_modes, patterns, specimen, offsets):
    modes, _, n, _ = probe_modes.shape
    count = patterns.shape[0]
    rows, cols = specimen.shape[1:]
    scan = lax.axis_size("scan")
    tile = lax.axis_size("tile")
    assert tile == 2 and scan % 2 == 0 and rows == n and modes % 2 == 0
    s = lax.axis_index("scan")
    t = lax.axis_index("tile")
    where = jnp.concatenate(
        [
            offsets[:, 0] - (s * rows - n),
            offsets[:, 1] - (t * cols - n),
            jnp.stack([s % 2, t]).astype(jnp.int32),
        ]
    )
    pairs = partners(scan, tile)
    strip = lax.dynamic_slice(specimen, (0, 0, (1 - t) * (cols - n)), (2, rows, n))
    side_b = lax.ppermute(specimen, AXES, pairs[1])
    strip_b = lax.ppermute(strip, AXES, pairs[4])
    strip_a = lax.ppermute(strip, AXES, pairs[3])
    strip_y = lax.ppermute(strip, AXES, pairs[2])
    side_a = lax.ppermute(specimen, AXES, pairs[0])

    wide = jax.ShapeDtypeStruct((3, rows, cols), f32)
    narrow = jax.ShapeDtypeStruct((3, rows, n), f32)
    planes = 2 * modes + 2
    ext_rows = rows + 2 * n + 8
    ext_cols = cols + 3 * n
    sums, fold_own, fold_a, fold_b, fold_y, fold_ya, fold_yb = pl.pallas_call(
        positions_kernel,
        out_shape=(
            jax.ShapeDtypeStruct((planes, n, n), f32), wide, wide, wide, narrow, narrow, narrow,
        ),
        in_specs=[pl.BlockSpec(memory_space=pltpu.SMEM)] + vmem(12),
        out_specs=tuple(vmem(7)),
        scratch_shapes=[
            pltpu.VMEM((2, ext_rows, ext_cols), f32),
            pltpu.VMEM((3, ext_rows, ext_cols), f32),
            pltpu.VMEM((modes // 2, 2 * n, 2 * n), f32),
            pltpu.VMEM((2, n, n), f32),
            pltpu.VMEM((n, n), f32),
            pltpu.VMEM((n, n), f32),
            pltpu.VMEM((2, n, n), f32),
        ],
        name="positions",
    )(
        where, probe_modes, patterns, specimen, side_a, side_b, strip_y, strip_a, strip_b,
        *dft_tables(n),
    )

    back_b = lax.ppermute(fold_b, AXES, pairs[1])
    back_yb = lax.ppermute(fold_yb, AXES, pairs[4])
    back_ya = lax.ppermute(fold_ya, AXES, pairs[3])
    back_y = lax.ppermute(fold_y, AXES, pairs[2])
    back_a = lax.ppermute(fold_a, AXES, pairs[0])

    half = n // 2
    pieces = tuple(sums[k, i * half : (i + 1) * half] for k in range(planes) for i in range(2))
    reduced = lax.psum((*pieces, sums[planes - 1, 0, 0]), AXES)[:-1]
    new_probe = pl.pallas_call(
        probe_kernel,
        out_shape=jax.ShapeDtypeStruct((2 * modes, n, n), f32),
        in_specs=vmem(1 + len(reduced)),
        out_specs=vmem(1)[0],
        scratch_shapes=[pltpu.VMEM((2 * modes, n, n), f32)],
        name="probe",
    )(probe_modes, *reduced)
    new_specimen = pl.pallas_call(
        object_kernel,
        out_shape=jax.ShapeDtypeStruct(specimen.shape, f32),
        in_specs=[pl.BlockSpec(memory_space=pltpu.SMEM)] + vmem(7),
        out_specs=vmem(1)[0],
        name="object",
    )(where, specimen, fold_own, back_a, back_b, back_y, back_ya, back_yb)
    return (new_probe.reshape(probe_modes.shape), new_specimen)


def solution(mesh):
    return jax.shard_map(
        body,
        mesh=mesh,
        in_specs=(
            P(),
            P(AXES, None, None),
            P(None, "scan", "tile"),
            P(AXES, None),
        ),
        out_specs=(P(), P(None, "scan", "tile")),
        check_vma=False,
    )
```

```python
import math

import jax
import jax.numpy as jnp
import numpy as np
from jax import lax
from jax.experimental import pallas as pl
from jax.experimental.pallas import tpu as pltpu
from jax.sharding import PartitionSpec as P


NS_STEPS = 8
AXES = ("scan", "tile")
light_floor = 0.05
object_reg = 0.5
probe_reg = 1.0
total_eps = 1e-06
f32 = jnp.float32
bf16 = jnp.bfloat16
highest = lax.Precision.HIGHEST


def dft_tables(detector):
    index = np.arange(detector, dtype=np.int64)
    angle = -2.0 * np.pi / detector * (index[:, None] * index[None, :] % detector)
    cos = np.cos(angle) / math.sqrt(detector)
    sin = np.sin(angle) / math.sqrt(detector)
    first = np.block([[cos, sin], [-sin, cos]]).astype(np.float32)
    second = np.block([[cos, -sin], [sin, cos]]).astype(np.float32)
    tables = []
    for table in (first, second):
        high = table.astype(bf16)
        low = (table - high.astype(np.float32)).astype(bf16)
        tables.append((high, low))
    (fh, fl), (sh, sl) = tables
    right_fwd = np.concatenate([fh, fh, fl], axis=0)
    right_inv = np.concatenate([sh, sh, sl], axis=0)
    left_fwd = np.concatenate([sh, sh, sl], axis=1)
    left_inv = np.concatenate([fh, fh, fl], axis=1)
    return tuple(jnp.asarray(t) for t in (right_fwd, left_fwd, right_inv, left_inv))


def split(values):
    high = values.astype(bf16)
    low = (values - high.astype(f32)).astype(bf16)
    return high, low


def right_product(rows, table):
    high, low = split(rows)
    return jnp.dot(jnp.concatenate([high, low, high], axis=1), table, preferred_element_type=f32)


def left_product(table, columns):
    high, low = split(columns)
    return jnp.dot(table, jnp.concatenate([high, low, high], axis=0), preferred_element_type=f32)


def to_columns(rows, n):
    top = jnp.concatenate([rows[:n, :n], rows[n:, :n]], axis=1)
    bottom = jnp.concatenate([rows[:n, n:], rows[n:, n:]], axis=1)
    return jnp.concatenate([top, bottom], axis=0)


def prepare_kernel(*refs):
    inputs, outputs, power, root, measured, done = refs[:7], refs[7:14], *refs[14:]
    copies = [
        pltpu.make_async_copy(src, dst, done.at[i])
        for i, (src, dst) in enumerate(zip(inputs, outputs))
    ]
    for copy in copies:
        copy.start()
    for copy in copies[:2]:
        copy.wait()
    probe, patterns = outputs[:2]
    modes, _, n, _ = probe.shape
    total = jnp.zeros((n, n), f32)
    for k in range(modes):
        total = total + probe[k, 0] * probe[k, 0] + probe[k, 1] * probe[k, 1]
    power[...] = total
    light = jnp.zeros((8, n), f32)
    for p in range(patterns.shape[0]):
        values = patterns[p]
        root[p] = jnp.sqrt(values)
        light = light + jnp.sum(values.reshape(n // 8, 8, n), axis=0)
    measured[...] = light
    for copy in copies[2:]:
        copy.wait()


def positions_kernel(
    where, probe, root, power, measured, own, side_a, side_b, strip_y, strip_a, strip_b,
    right_fwd, left_fwd, right_inv, left_inv,
    *refs,
):
    parts = refs[: 2 * PARTS]
    fold_own, fold_a, fold_b, fold_y, fold_ya, fold_yb = refs[2 * PARTS : 2 * PARTS + 6]
    sums, extended, frame, far, patch, model, numer = refs[2 * PARTS + 6 :]
    modes, _, n, _ = probe.shape
    count = root.shape[0]
    rows, cols = own.shape[1:]
    even = where[2 * count] == 0
    first_tile = where[2 * count + 1] == 0
    row_a = pl.multiple_of(jnp.where(even, n + rows, 0), n)
    row_b = pl.multiple_of(jnp.where(even, 0, n + rows), n)
    col_y = pl.multiple_of(jnp.where(first_tile, n + cols, 0), n)
    col_z = pl.multiple_of(jnp.where(first_tile, 0, n + cols), n)

    frame[...] = jnp.zeros_like(frame)
    extended[:, :, pl.ds(col_z, n)] = jnp.zeros((2, extended.shape[1], n), f32)
    extended[:, n : n + rows, n : n + cols] = own[...]
    extended[:, pl.ds(row_a, n), n : n + cols] = side_a[...]
    extended[:, pl.ds(row_b, n), n : n + cols] = side_b[...]
    extended[:, n : n + rows, pl.ds(col_y, n)] = strip_y[...]
    extended[:, pl.ds(row_a, n), pl.ds(col_y, n)] = strip_a[...]
    extended[:, pl.ds(row_b, n), pl.ds(col_y, n)] = strip_b[...]

    sums[...] = jnp.zeros_like(sums)
    sums[2 * modes + 1, 8:16] = measured[...]
    pairs = modes // 2

    def one_position(p, carry):
        row = where[p]
        col = where[count + p]
        col_block = pl.multiple_of(col // n * n, n)
        shift = col - col_block
        row_block = pl.multiple_of(row // 8 * 8, 8)
        down = row - row_block
        for c in range(2):
            window = extended[c, pl.ds(row_block, n + 8), pl.ds(col_block, 2 * n)]
            window = pltpu.roll(window, (2 * n - shift) % (2 * n), 1)[:, :n]
            patch[c] = pltpu.roll(window, (n + 8 - down) % (n + 8), 0)[:n]
        model[...] = jnp.zeros_like(model)

        def forward(q, carry):
            p_re = patch[0]
            p_im = patch[1]
            blocks = []
            for k in range(2):
                re = probe[2 * q + k, 0]
                im = probe[2 * q + k, 1]
                blocks.append(
                    jnp.concatenate([re * p_re - im * p_im, re * p_im + im * p_re], axis=1)
                )
            half = right_product(jnp.concatenate(blocks, axis=0), right_fwd[...])
            full = left_product(left_fwd[...], to_columns(half, n))
            far[q] = full
            squares = full * full
            squares = squares[:n] + squares[n:]
            model[...] += squares[:, :n] + squares[:, n:]
            return carry

        lax.fori_loop(0, pairs, forward, 0, unroll=UNROLL)
        light = model[...]
        factor = root[p] / jnp.sqrt(jnp.maximum(light, light_floor)) - 1.0
        model[...] = factor
        sums[2 * modes + 1, 0:8] += jnp.sum(light.reshape(n // 8, 8, n), axis=0)
        numer[...] = jnp.zeros_like(numer)

        def backward(q, carry):
            factor = model[...]
            factor4 = jnp.concatenate([factor, factor], axis=1)
            factor4 = jnp.concatenate([factor4, factor4], axis=0)
            half = right_product(to_columns(far[q] * factor4, n), right_inv[...])
            change = left_product(left_inv[...], to_columns(half, n))
            p_re = patch[0]
            p_im = patch[1]
            num_re = numer[0]
            num_im = numer[1]
            for k in range(2):
                c_re = change[:n, k * n : (k + 1) * n]
                c_im = change[n:, k * n : (k + 1) * n]
                re = probe[2 * q + k, 0]
                im = probe[2 * q + k, 1]
                at = 4 * q + 2 * k
                sums[at] += p_re * c_re + p_im * c_im
                sums[at + 1] += p_re * c_im - p_im * c_re
                num_re = num_re + (re * c_re + im * c_im)
                num_im = num_im + (re * c_im - im * c_re)
            numer[0] = num_re
            numer[1] = num_im
            return carry

        lax.fori_loop(0, pairs, backward, 0, unroll=UNROLL)
        sums[2 * modes] += patch[0] * patch[0] + patch[1] * patch[1]
        for c in range(3):
            value = power[...] if c == 2 else numer[c]
            tall = pltpu.roll(jnp.concatenate([value, jnp.zeros((8, n), f32)], axis=0), down, 0)
            wide = pltpu.roll(jnp.concatenate([tall, jnp.zeros_like(tall)], axis=1), shift, 1)
            frame[c, pl.ds(row_block, n + 8), pl.ds(col_block, 2 * n)] += wide
        return carry

    lax.fori_loop(0, count, one_position, 0)
    half_rows = n // 2
    core = where[2 * count]
    mine = pl.multiple_of(core * half_rows, half_rows)
    theirs = pl.multiple_of((1 - core) * half_rows, half_rows)
    for h, (keep, send) in enumerate(zip(parts[0::2], parts[1::2])):
        planes = keep.shape[0]
        keep[...] = sums[h * planes : (h + 1) * planes, pl.ds(mine, half_rows)]
        send[...] = sums[h * planes : (h + 1) * planes, pl.ds(theirs, half_rows)]
    fold_own[...] = frame[:, n : n + rows, n : n + cols]
    fold_a[...] = frame[:, pl.ds(row_a, n), n : n + cols]
    fold_b[...] = frame[:, pl.ds(row_b, n), n : n + cols]
    fold_y[...] = frame[:, n : n + rows, pl.ds(col_y, n)]
    fold_ya[...] = frame[:, pl.ds(row_a, n), pl.ds(col_y, n)]
    fold_yb[...] = frame[:, pl.ds(row_b, n), pl.ds(col_y, n)]


UNROLL = 6
PARTS = 2


def object_kernel(where, specimen, own, side_a, side_b, strip_y, strip_a, strip_b, out):
    n = strip_y.shape[2]
    cols = own.shape[2]
    first_tile = where[where.shape[0] - 2] == 0
    at = pl.multiple_of(jnp.where(first_tile, cols - n, 0), n)
    own[...] += side_a[...] + side_b[...]
    own[:, :, pl.ds(at, n)] += strip_y[...] + strip_a[...] + strip_b[...]
    light = own[2] + object_reg
    out[0] = specimen[0] + own[0] / light
    out[1] = specimen[1] + own[1] / light


def split_kernel(where, keep, received, *outs):
    quarter = where[where.shape[0] - 1]
    rows = outs[0].shape[1]
    for k, out in enumerate(outs):
        at = pl.ds(pl.multiple_of((quarter ^ k) * rows, rows), rows)
        out[...] = keep[:, at] + received[:, at]


def join_kernel(where, *refs):
    quarter = where[where.shape[0] - 1]
    out = refs[-1]
    rows = refs[0].shape[1]
    for k, ref in enumerate(refs[:-1]):
        out[:, pl.ds(pl.multiple_of((quarter ^ k) * rows, rows), rows)] = ref[...]


def probe_kernel(where, probe, *refs):
    parts = refs[: 2 * PARTS]
    out, updated, sums, result, wide, done = refs[2 * PARTS :]
    modes, _, n, _ = probe.shape
    planes = 2 * modes
    half_rows = n // 2
    core = where[where.shape[0] - 3]
    mine = pl.multiple_of(core * half_rows, half_rows)
    theirs = pl.multiple_of((1 - core) * half_rows, half_rows)
    for h, (own, mate) in enumerate(zip(parts[0::2], parts[1::2])):
        part = own.shape[0]
        sums[h * part : (h + 1) * part, pl.ds(mine, half_rows)] = own[...]
        sums[h * part : (h + 1) * part, pl.ds(theirs, half_rows)] = mate[...]
    scale = 1.0 / (sums[planes] + probe_reg)

    def update(k, carry):
        for c in range(2):
            updated[2 * k + c] = probe[k, c] + sums[2 * k + c] * scale
        return carry

    lax.fori_loop(0, modes, update, 0)
    for k in range(planes, updated.shape[0]):
        updated[k] = jnp.zeros((n, n), f32)
    model_all = jnp.sum(sums[planes + 1, 0:8], keepdims=True)
    measured_all = jnp.sum(sums[planes + 1, 8:16], keepdims=True)
    ratio = measured_all / (model_all + total_eps)

    def rows_of(x, count):
        blocks = [
            updated[0:count, pl.ds(pl.multiple_of(x + i, 8), 8), :].reshape(8 * count, n)
            for i in (0, 8)
        ]
        return jnp.concatenate(blocks, axis=1)

    def mul(a, b):
        return jnp.dot(a, b, precision=highest, preferred_element_type=f32)

    tall = 8 * planes
    wide[...] = jnp.zeros_like(wide)

    def accumulate(b, carry):
        left, right = [], []
        for x in (0, 16):
            high, low = split(rows_of(32 * b + x, planes))
            left += [high, low, high, low]
            right += [high, high, low, low]
        wide[...] += lax.dot_general(
            jnp.concatenate(left, axis=1),
            jnp.concatenate(right, axis=1),
            (((1,), (1,)), ((), ())),
            preferred_element_type=f32,
        )
        return carry

    lax.fori_loop(0, n // 32, accumulate, 0, unroll=4)
    wide_gram = wide[...]
    r0 = lax.broadcasted_iota(jnp.int32, (tall, tall), 0)
    r1 = lax.broadcasted_iota(jnp.int32, (tall, tall), 1)
    same_row = r0 % 8 == r1 % 8
    spread = jnp.where(
        lax.broadcasted_iota(jnp.int32, (tall, planes), 0) // 8
        == lax.broadcasted_iota(jnp.int32, (tall, planes), 1),
        1.0,
        0.0,
    )
    gather = jnp.where(
        lax.broadcasted_iota(jnp.int32, (planes, tall), 1) // 8
        == lax.broadcasted_iota(jnp.int32, (planes, tall), 0),
        1.0,
        0.0,
    )
    i0 = lax.broadcasted_iota(jnp.int32, (planes, planes), 0)
    i1 = lax.broadcasted_iota(jnp.int32, (planes, planes), 1)
    identity = jnp.where(i0 == i1, 1.0, 0.0)

    def turned(lead, follow):
        up = jnp.where(lead == follow + 1, jnp.where(follow % 2 == 0, 1.0, 0.0), 0.0)
        return up - jnp.where(follow == lead + 1, jnp.where(lead % 2 == 0, 1.0, 0.0), 0.0)

    spread_turned = turned(
        lax.broadcasted_iota(jnp.int32, (tall, planes), 0) // 8,
        lax.broadcasted_iota(jnp.int32, (tall, planes), 1),
    )
    gather_turned = turned(
        lax.broadcasted_iota(jnp.int32, (planes, tall), 0),
        lax.broadcasted_iota(jnp.int32, (planes, tall), 1) // 8,
    )
    wide_gram = jnp.where(same_row, wide_gram, 0.0)
    hermitian = mul(gather, mul(wide_gram, spread)) - mul(
        gather_turned, mul(wide_gram, spread_turned)
    )
    frobenius = jnp.sqrt(jnp.sum(hermitian * hermitian, keepdims=True))

    def newton(_, carry):
        current, inverse = carry
        factor = 1.5 * identity - 0.5 * mul(inverse, current)
        return mul(current, factor), mul(factor, inverse)

    _, inverse = lax.fori_loop(0, NS_STEPS, newton, (hermitian / frobenius, identity))
    inverse = inverse / jnp.sqrt(frobenius)
    diagonal = jnp.sum(hermitian * identity, axis=1, keepdims=True)
    mix = inverse * jnp.sqrt(ratio * diagonal)
    full = 8 * updated.shape[0]

    def rows8(values):
        return jnp.broadcast_to(values[:, None, :], (planes, 8, tall)).reshape(tall, tall)

    wide_mix = jnp.where(same_row, rows8(mul(mix, gather)), 0.0)
    wide_mix = jnp.concatenate([wide_mix, jnp.zeros((tall, full - tall), f32)], axis=1)
    high, low = split(wide_mix)
    table = jnp.concatenate([high, high, low], axis=1)

    def out_copy(b):
        at = pl.ds(pl.multiple_of(32 * b, 32), 32)
        return pltpu.make_async_copy(result.at[:, at, :], out.at[:, at, :], done.at[b])

    def orthogonalize(b, carry):
        for x in (0, 16):
            mixed = left_product(table, rows_of(32 * b + x, updated.shape[0]))
            for i in range(2):
                at = pl.ds(pl.multiple_of(32 * b + x + 8 * i, 8), 8)
                result[:, at, :] = mixed[:, i * n : (i + 1) * n].reshape(planes, 8, n)
        out_copy(b).start()
        return carry

    lax.fori_loop(0, n // 32, orthogonalize, 0, unroll=4)

    def drain(b, carry):
        out_copy(b).wait()
        return carry

    lax.fori_loop(0, n // 32, drain, 0)


def vmem(count):
    return [pl.BlockSpec(memory_space=pltpu.VMEM)] * count


def on_chip(*arrays):
    return tuple(pltpu.with_memory_space_constraint(a, pltpu.VMEM) for a in arrays)


def limit(mib):
    return pltpu.CompilerParams(vmem_limit_bytes=mib * 2**20)


def partners(scan, tile):
    def flat(s, t):
        return s * tile + t

    mates, others, across, mates_across, others_across = [], [], [], [], []
    for s in range(scan):
        mate = s ^ 1
        other = s + 1 if s % 2 else s - 1
        for t in range(tile):
            here = flat(s, t)
            mates.append((here, flat(mate, t)))
            across.append((here, flat(s, 1 - t)))
            mates_across.append((here, flat(mate, 1 - t)))
            if 0 <= other < scan:
                others.append((here, flat(other, t)))
                others_across.append((here, flat(other, 1 - t)))
    return mates, others, across, mates_across, others_across


def send(array, pairs):
    return lax.ppermute(array, AXES, pairs)


def peers(scan, tile, scan_flip, tile_flip):
    return [
        (s * tile + t, (s ^ scan_flip) * tile + (t ^ tile_flip))
        for s in range(scan)
        for t in range(tile)
    ]


def probe_update(where, probe_chip, keeps, sends, mates, scan, tile):
    modes, _, n, _ = probe_chip.shape
    group = [peers(scan, tile, 2 * (k // 2), k % 2) for k in range(1, 4)]
    smem = pl.BlockSpec(memory_space=pltpu.SMEM)
    joined = []
    for keep, other in zip(keeps, sends):
        planes, rows, _ = keep.shape
        received = send(other, mates)
        block = pltpu.VMEM((planes, rows // 4, n), f32)
        own, *others = pl.pallas_call(
            split_kernel,
            out_shape=(block,) * 4,
            in_specs=[smem] + vmem(2),
            out_specs=tuple(vmem(4)),
            name="split",
        compiler_params=limit(4),
        )(where, *on_chip(keep, received))
        total = own
        arrived = [send(other, perm) for other, perm in zip(others, group)]
        total = own + arrived[0] + arrived[1] + arrived[2]
        flip = 4
        while flip < scan:
            total = total + send(total, peers(scan, tile, 2 * flip - 4, 0))
            flip = flip * 2
        arrived = [send(total, perm) for perm in group]
        mine = pl.pallas_call(
            join_kernel,
            out_shape=pltpu.VMEM(keep.shape, f32),
            in_specs=[smem] + vmem(4),
            out_specs=vmem(1)[0],
            name="join",
        compiler_params=limit(4),
        )(where, *on_chip(total, *arrived))
        joined += [mine, send(mine, mates)]
    planes = 2 * modes
    return pl.pallas_call(
        probe_kernel,
        out_shape=jax.ShapeDtypeStruct((planes, n, n), f32),
        in_specs=[smem] + vmem(1 + 2 * PARTS),
        out_specs=pl.BlockSpec(memory_space=pl.ANY),
        scratch_shapes=[
            pltpu.VMEM((-(-planes // 32) * 32, n, n), f32),
            pltpu.VMEM((planes + 2, n, n), f32),
            pltpu.VMEM((planes, n, n), f32),
            pltpu.VMEM((8 * planes, 8 * planes), f32),
            pltpu.SemaphoreType.DMA((n // 32,)),
        ],
        name="probe",
        compiler_params=limit(20),
    )(where, *on_chip(probe_chip, *joined))


def program(probe_modes, patterns, specimen, offsets):
    modes, _, n, _ = probe_modes.shape
    count = patterns.shape[0]
    rows, cols = specimen.shape[1:]
    scan = lax.axis_size("scan")
    tile = lax.axis_size("tile")
    assert tile == 2 and scan >= 4 and scan & (scan - 1) == 0 and rows == n and modes % 2 == 0
    s = lax.axis_index("scan")
    t = lax.axis_index("tile")
    where = jnp.concatenate(
        [
            offsets[:, 0] - (s * rows - n),
            offsets[:, 1] - (t * cols - n),
            jnp.stack([s % 2, t, s // 2 % 2 * 2 + t]).astype(jnp.int32),
        ]
    )
    pairs = partners(scan, tile)
    strip = lax.dynamic_slice(specimen, (0, 0, (1 - t) * (cols - n)), (2, rows, n))
    side_b = send(specimen, pairs[1])
    strip_b = send(strip, pairs[4])
    strip_y = send(strip, pairs[2])
    strip_a = send(strip, pairs[3])
    side_a = send(specimen, pairs[0])

    inputs = (probe_modes, patterns, specimen, *dft_tables(n))
    probe_chip, _, own, *tables, power, root, measured = pl.pallas_call(
        prepare_kernel,
        out_shape=tuple(pltpu.VMEM(a.shape, a.dtype) for a in inputs)
        + (
            pltpu.VMEM((n, n), f32), pltpu.VMEM((count, n, n), f32), pltpu.VMEM((8, n), f32),
        ),
        in_specs=[pl.BlockSpec(memory_space=pltpu.HBM)] * 7,
        out_specs=tuple(vmem(10)),
        scratch_shapes=[pltpu.SemaphoreType.DMA((7,))],
        name="prepare",
        compiler_params=limit(8),
    )(*(pltpu.with_memory_space_constraint(a, pltpu.HBM) for a in inputs))

    wide = pltpu.VMEM((3, rows, cols), f32)
    narrow = pltpu.VMEM((3, rows, n), f32)
    planes = 2 * modes + 2
    ext_rows = rows + 2 * n + 8
    ext_cols = cols + 3 * n
    part = pltpu.VMEM((planes // PARTS, n // 2, n), f32)
    *halves, fold_own, fold_a, fold_b, fold_y, fold_ya, fold_yb = pl.pallas_call(
        positions_kernel,
        out_shape=(part,) * (2 * PARTS) + (wide, wide, wide, narrow, narrow, narrow),
        in_specs=[pl.BlockSpec(memory_space=pltpu.SMEM)] + vmem(14),
        out_specs=tuple(vmem(6 + 2 * PARTS)),
        scratch_shapes=[
            pltpu.VMEM((planes, n, n), f32),
            pltpu.VMEM((2, ext_rows, ext_cols), f32),
            pltpu.VMEM((3, ext_rows, ext_cols), f32),
            pltpu.VMEM((modes // 2, 2 * n, 2 * n), f32),
            pltpu.VMEM((2, n, n), f32),
            pltpu.VMEM((n, n), f32),
            pltpu.VMEM((2, n, n), f32),
        ],
        name="positions",
        compiler_params=limit(30),
    )(
        where,
        *on_chip(
            probe_chip, root, power, measured, own, side_a, side_b, strip_y, strip_a, strip_b,
            *tables,
        ),
    )

    keeps, sends = halves[0::2], halves[1::2]
    back_b = send(fold_b, pairs[1])
    back_yb = send(fold_yb, pairs[4])
    back_y = send(fold_y, pairs[2])
    back_ya = send(fold_ya, pairs[3])
    back_a = send(fold_a, pairs[0])

    new_probe = probe_update(where, probe_chip, keeps, sends, pairs[0], scan, tile)
    new_specimen = finish(where, own, fold_own, back_a, back_b, back_y, back_ya, back_yb)
    return (new_probe.reshape(probe_modes.shape), new_specimen)


def finish(where, own, *folds):
    return pl.pallas_call(
        object_kernel,
        out_shape=jax.ShapeDtypeStruct(own.shape, f32),
        in_specs=[pl.BlockSpec(memory_space=pltpu.SMEM)] + vmem(7),
        out_specs=vmem(1)[0],
        name="object",
        compiler_params=limit(4),
    )(where, *on_chip(own, *folds))


def solution(mesh):
    return jax.shard_map(
        program,
        mesh=mesh,
        in_specs=(
            P(),
            P(AXES, None, None),
            P(None, "scan", "tile"),
            P(AXES, None),
        ),
        out_specs=(P(), P(None, "scan", "tile")),
        check_vma=False,
    )
```

```python
import math

import jax
import jax.numpy as jnp
import numpy as np
from jax import lax
from jax.experimental import pallas as pl
from jax.experimental.pallas import tpu as pltpu
from jax.sharding import PartitionSpec as P


NS_STEPS = 8
AXES = ("scan", "tile")
light_floor = 0.05
object_reg = 0.5
probe_reg = 1.0
total_eps = 1e-06
f32 = jnp.float32
bf16 = jnp.bfloat16
highest = lax.Precision.HIGHEST


def dft_tables(detector):
    index = np.arange(detector, dtype=np.int64)
    angle = -2.0 * np.pi / detector * (index[:, None] * index[None, :] % detector)
    cos = np.cos(angle) / math.sqrt(detector)
    sin = np.sin(angle) / math.sqrt(detector)
    first = np.block([[cos, sin], [-sin, cos]]).astype(np.float32)
    second = np.block([[cos, -sin], [sin, cos]]).astype(np.float32)
    tables = []
    for table in (first, second):
        high = table.astype(bf16)
        low = (table - high.astype(np.float32)).astype(bf16)
        tables.append((high, low))
    (fh, fl), (sh, sl) = tables
    right_fwd = np.concatenate([fh, fh, fl], axis=0)
    right_inv = np.concatenate([sh, sh, sl], axis=0)
    left_fwd = np.concatenate([sh, sh, sl], axis=1)
    left_inv = np.concatenate([fh, fh, fl], axis=1)
    return tuple(jnp.asarray(t) for t in (right_fwd, left_fwd, right_inv, left_inv))


def split(values):
    high = values.astype(bf16)
    low = (values - high.astype(f32)).astype(bf16)
    return high, low


def right_product(rows, table):
    high, low = split(rows)
    return jnp.dot(jnp.concatenate([high, low, high], axis=1), table, preferred_element_type=f32)


def left_product(table, columns):
    high, low = split(columns)
    return jnp.dot(table, jnp.concatenate([high, low, high], axis=0), preferred_element_type=f32)


def to_columns(rows, n):
    top = jnp.concatenate([rows[:n, :n], rows[n:, :n]], axis=1)
    bottom = jnp.concatenate([rows[:n, n:], rows[n:, n:]], axis=1)
    return jnp.concatenate([top, bottom], axis=0)


def prepare_kernel(*refs):
    inputs, outputs, power, root, measured, done = refs[:7], refs[7:14], *refs[14:]
    copies = [
        pltpu.make_async_copy(src, dst, done.at[i])
        for i, (src, dst) in enumerate(zip(inputs, outputs))
    ]
    for copy in copies:
        copy.start()
    for copy in copies[:2]:
        copy.wait()
    probe, patterns = outputs[:2]
    modes, _, n, _ = probe.shape
    total = jnp.zeros((n, n), f32)
    for k in range(modes):
        total = total + probe[k, 0] * probe[k, 0] + probe[k, 1] * probe[k, 1]
    power[...] = total
    light = jnp.zeros((8, n), f32)
    for p in range(patterns.shape[0]):
        values = patterns[p]
        root[p] = jnp.sqrt(values)
        light = light + jnp.sum(values.reshape(n // 8, 8, n), axis=0)
    measured[...] = light
    for copy in copies[2:]:
        copy.wait()


def positions_kernel(
    where, probe, root, power, measured, own, side_a, side_b, strip_y, strip_a, strip_b,
    right_fwd, left_fwd, right_inv, left_inv,
    *refs,
):
    parts = refs[: 2 * PARTS]
    fold_own, fold_a, fold_b, fold_y = refs[2 * PARTS : 2 * PARTS + 4]
    sums, extended, frame, far, patch, model, numer = refs[2 * PARTS + 4 :]
    modes, _, n, _ = probe.shape
    count = root.shape[0]
    rows, cols = own.shape[1:]
    even = where[2 * count] == 0
    first_tile = where[2 * count + 1] == 0
    row_a = pl.multiple_of(jnp.where(even, n + rows, 0), n)
    row_b = pl.multiple_of(jnp.where(even, 0, n + rows), n)
    col_y = pl.multiple_of(jnp.where(first_tile, n + cols, 0), n)
    col_z = pl.multiple_of(jnp.where(first_tile, 0, n + cols), n)

    frame[...] = jnp.zeros_like(frame)
    extended[:, :, pl.ds(col_z, n)] = jnp.zeros((2, extended.shape[1], n), f32)
    extended[:, n : n + rows, n : n + cols] = own[...]
    extended[:, pl.ds(row_a, n), n : n + cols] = side_a[...]
    extended[:, pl.ds(row_b, n), n : n + cols] = side_b[...]
    extended[:, n : n + rows, pl.ds(col_y, n)] = strip_y[...]
    extended[:, pl.ds(row_a, n), pl.ds(col_y, n)] = strip_a[...]
    extended[:, pl.ds(row_b, n), pl.ds(col_y, n)] = strip_b[...]

    sums[...] = jnp.zeros_like(sums)
    sums[2 * modes + 1, 8:16] = measured[...]
    pairs = modes // 2

    def one_position(p, carry):
        row = where[p]
        col = where[count + p]
        col_block = pl.multiple_of(col // n * n, n)
        shift = col - col_block
        row_block = pl.multiple_of(row // 8 * 8, 8)
        down = row - row_block
        for c in range(2):
            window = extended[c, pl.ds(row_block, n + 8), pl.ds(col_block, 2 * n)]
            window = pltpu.roll(window, (2 * n - shift) % (2 * n), 1)[:, :n]
            patch[c] = pltpu.roll(window, (n + 8 - down) % (n + 8), 0)[:n]
        model[...] = jnp.zeros_like(model)

        def forward(q, carry):
            p_re = patch[0]
            p_im = patch[1]
            blocks = []
            for k in range(2):
                re = probe[2 * q + k, 0]
                im = probe[2 * q + k, 1]
                blocks.append(
                    jnp.concatenate([re * p_re - im * p_im, re * p_im + im * p_re], axis=1)
                )
            half = right_product(jnp.concatenate(blocks, axis=0), right_fwd[...])
            full = left_product(left_fwd[...], to_columns(half, n))
            far[q] = full
            squares = full * full
            squares = squares[:n] + squares[n:]
            model[...] += squares[:, :n] + squares[:, n:]
            return carry

        lax.fori_loop(0, pairs, forward, 0, unroll=UNROLL)
        light = model[...]
        factor = root[p] / jnp.sqrt(jnp.maximum(light, light_floor)) - 1.0
        model[...] = factor
        sums[2 * modes + 1, 0:8] += jnp.sum(light.reshape(n // 8, 8, n), axis=0)
        numer[...] = jnp.zeros_like(numer)

        def backward(q, carry):
            factor = model[...]
            factor4 = jnp.concatenate([factor, factor], axis=1)
            factor4 = jnp.concatenate([factor4, factor4], axis=0)
            half = right_product(to_columns(far[q] * factor4, n), right_inv[...])
            change = left_product(left_inv[...], to_columns(half, n))
            p_re = patch[0]
            p_im = patch[1]
            num_re = numer[0]
            num_im = numer[1]
            for k in range(2):
                c_re = change[:n, k * n : (k + 1) * n]
                c_im = change[n:, k * n : (k + 1) * n]
                re = probe[2 * q + k, 0]
                im = probe[2 * q + k, 1]
                at = 4 * q + 2 * k
                sums[at] += p_re * c_re + p_im * c_im
                sums[at + 1] += p_re * c_im - p_im * c_re
                num_re = num_re + (re * c_re + im * c_im)
                num_im = num_im + (re * c_im - im * c_re)
            numer[0] = num_re
            numer[1] = num_im
            return carry

        lax.fori_loop(0, pairs, backward, 0, unroll=UNROLL)
        sums[2 * modes] += patch[0] * patch[0] + patch[1] * patch[1]
        for c in range(3):
            value = power[...] if c == 2 else numer[c]
            tall = pltpu.roll(jnp.concatenate([value, jnp.zeros((8, n), f32)], axis=0), down, 0)
            wide = pltpu.roll(jnp.concatenate([tall, jnp.zeros_like(tall)], axis=1), shift, 1)
            frame[c, pl.ds(row_block, n + 8), pl.ds(col_block, 2 * n)] += wide
        return carry

    lax.fori_loop(0, count, one_position, 0)
    half_rows = n // 2
    core = where[2 * count]
    mine = pl.multiple_of(core * half_rows, half_rows)
    theirs = pl.multiple_of((1 - core) * half_rows, half_rows)
    for h, (keep, send) in enumerate(zip(parts[0::2], parts[1::2])):
        planes = keep.shape[0]
        keep[...] = sums[h * planes : (h + 1) * planes, pl.ds(mine, half_rows)]
        send[...] = sums[h * planes : (h + 1) * planes, pl.ds(theirs, half_rows)]
    fold_own[...] = frame[:, n : n + rows, n : n + cols]
    fold_a[...] = frame[:, pl.ds(row_a, n), n : n + cols]
    fold_b[...] = frame[:, pl.ds(row_b, n), n : n + cols]
    fold_y[0] = frame[:, n : n + rows, pl.ds(col_y, n)]
    fold_y[1] = frame[:, pl.ds(row_a, n), pl.ds(col_y, n)]
    fold_y[2] = frame[:, pl.ds(row_b, n), pl.ds(col_y, n)]


UNROLL = 6
PARTS = 2


def edge_kernel(where, column, *refs):
    n = column.shape[3]
    cols = refs[0].shape[2]
    first_tile = where[where.shape[0] - 2] == 0
    at = pl.multiple_of(jnp.where(first_tile, cols - n, 0), n)
    for k in range(3):
        out = refs[3 + k]
        out[...] = refs[k][...]
        out[:, :, pl.ds(at, n)] += column[k]


def object_kernel(specimen, own, side_a, side_b, after, out):
    total = own[...] + side_a[...] + side_b[...]
    light = total[2] + object_reg
    out[0] = specimen[0] + total[0] / light
    out[1] = specimen[1] + total[1] / light


def split_kernel(where, keep, received, *outs):
    quarter = where[where.shape[0] - 1]
    rows = outs[0].shape[1]
    for k, out in enumerate(outs):
        at = pl.ds(pl.multiple_of((quarter ^ k) * rows, rows), rows)
        out[...] = keep[:, at] + received[:, at]


def join_kernel(where, *refs):
    quarter = where[where.shape[0] - 1]
    out = refs[-1]
    rows = refs[0].shape[1]
    for k, ref in enumerate(refs[:-1]):
        out[:, pl.ds(pl.multiple_of((quarter ^ k) * rows, rows), rows)] = ref[...]


def probe_kernel(where, probe, *refs):
    parts = refs[: 2 * PARTS]
    out, updated, sums, result, wide, done = refs[2 * PARTS :]
    modes, _, n, _ = probe.shape
    planes = 2 * modes
    half_rows = n // 2
    core = where[where.shape[0] - 3]
    mine = pl.multiple_of(core * half_rows, half_rows)
    theirs = pl.multiple_of((1 - core) * half_rows, half_rows)
    for h, (own, mate) in enumerate(zip(parts[0::2], parts[1::2])):
        part = own.shape[0]
        sums[h * part : (h + 1) * part, pl.ds(mine, half_rows)] = own[...]
        sums[h * part : (h + 1) * part, pl.ds(theirs, half_rows)] = mate[...]
    scale = 1.0 / (sums[planes] + probe_reg)

    def update(k, carry):
        for c in range(2):
            updated[2 * k + c] = probe[k, c] + sums[2 * k + c] * scale
        return carry

    lax.fori_loop(0, modes, update, 0)
    for k in range(planes, updated.shape[0]):
        updated[k] = jnp.zeros((n, n), f32)
    model_all = jnp.sum(sums[planes + 1, 0:8], keepdims=True)
    measured_all = jnp.sum(sums[planes + 1, 8:16], keepdims=True)
    ratio = measured_all / (model_all + total_eps)

    def rows_of(x, count):
        blocks = [
            updated[0:count, pl.ds(pl.multiple_of(x + i, 8), 8), :].reshape(8 * count, n)
            for i in (0, 8)
        ]
        return jnp.concatenate(blocks, axis=1)

    def mul(a, b):
        return jnp.dot(a, b, precision=highest, preferred_element_type=f32)

    tall = 8 * planes
    wide[...] = jnp.zeros_like(wide)

    def accumulate(b, carry):
        left, right = [], []
        for x in (0, 16):
            high, low = split(rows_of(32 * b + x, planes))
            left += [high, low, high, low]
            right += [high, high, low, low]
        wide[...] += lax.dot_general(
            jnp.concatenate(left, axis=1),
            jnp.concatenate(right, axis=1),
            (((1,), (1,)), ((), ())),
            preferred_element_type=f32,
        )
        return carry

    lax.fori_loop(0, n // 32, accumulate, 0, unroll=4)
    wide_gram = wide[...]
    r0 = lax.broadcasted_iota(jnp.int32, (tall, tall), 0)
    r1 = lax.broadcasted_iota(jnp.int32, (tall, tall), 1)
    same_row = r0 % 8 == r1 % 8
    spread = jnp.where(
        lax.broadcasted_iota(jnp.int32, (tall, planes), 0) // 8
        == lax.broadcasted_iota(jnp.int32, (tall, planes), 1),
        1.0,
        0.0,
    )
    gather = jnp.where(
        lax.broadcasted_iota(jnp.int32, (planes, tall), 1) // 8
        == lax.broadcasted_iota(jnp.int32, (planes, tall), 0),
        1.0,
        0.0,
    )
    i0 = lax.broadcasted_iota(jnp.int32, (planes, planes), 0)
    i1 = lax.broadcasted_iota(jnp.int32, (planes, planes), 1)
    identity = jnp.where(i0 == i1, 1.0, 0.0)

    def turned(lead, follow):
        up = jnp.where(lead == follow + 1, jnp.where(follow % 2 == 0, 1.0, 0.0), 0.0)
        return up - jnp.where(follow == lead + 1, jnp.where(lead % 2 == 0, 1.0, 0.0), 0.0)

    spread_turned = turned(
        lax.broadcasted_iota(jnp.int32, (tall, planes), 0) // 8,
        lax.broadcasted_iota(jnp.int32, (tall, planes), 1),
    )
    gather_turned = turned(
        lax.broadcasted_iota(jnp.int32, (planes, tall), 0),
        lax.broadcasted_iota(jnp.int32, (planes, tall), 1) // 8,
    )
    wide_gram = jnp.where(same_row, wide_gram, 0.0)
    hermitian = mul(gather, mul(wide_gram, spread)) - mul(
        gather_turned, mul(wide_gram, spread_turned)
    )
    frobenius = jnp.sqrt(jnp.sum(hermitian * hermitian, keepdims=True))

    def newton(_, carry):
        current, inverse = carry
        factor = 1.5 * identity - 0.5 * mul(inverse, current)
        return mul(current, factor), mul(factor, inverse)

    current = hermitian / frobenius
    factor = 1.5 * identity - 0.5 * current
    _, inverse = lax.fori_loop(1, NS_STEPS, newton, (mul(current, factor), factor))
    inverse = inverse / jnp.sqrt(frobenius)
    diagonal = jnp.sum(hermitian * identity, axis=1, keepdims=True)
    mix = inverse * jnp.sqrt(ratio * diagonal)
    full = 8 * updated.shape[0]

    def rows8(values):
        return jnp.broadcast_to(values[:, None, :], (planes, 8, tall)).reshape(tall, tall)

    wide_mix = jnp.where(same_row, rows8(mul(mix, gather)), 0.0)
    wide_mix = jnp.concatenate([wide_mix, jnp.zeros((tall, full - tall), f32)], axis=1)
    high, low = split(wide_mix)
    table = jnp.concatenate([high, high, low], axis=1)

    def out_copy(b):
        at = pl.ds(pl.multiple_of(32 * b, 32), 32)
        return pltpu.make_async_copy(result.at[:, at, :], out.at[:, at, :], done.at[b])

    def orthogonalize(b, carry):
        for x in (0, 16):
            mixed = left_product(table, rows_of(32 * b + x, updated.shape[0]))
            for i in range(2):
                at = pl.ds(pl.multiple_of(32 * b + x + 8 * i, 8), 8)
                result[:, at, :] = mixed[:, i * n : (i + 1) * n].reshape(planes, 8, n)
        out_copy(b).start()
        return carry

    lax.fori_loop(0, n // 32, orthogonalize, 0, unroll=4)

    def drain(b, carry):
        out_copy(b).wait()
        return carry

    lax.fori_loop(0, n // 32, drain, 0)


def vmem(count):
    return [pl.BlockSpec(memory_space=pltpu.VMEM)] * count


def on_chip(*arrays):
    return tuple(pltpu.with_memory_space_constraint(a, pltpu.VMEM) for a in arrays)


def limit(mib):
    return pltpu.CompilerParams(vmem_limit_bytes=mib * 2**20)


def partners(scan, tile):
    def flat(s, t):
        return s * tile + t

    mates, others, across, mates_across, others_across = [], [], [], [], []
    for s in range(scan):
        mate = s ^ 1
        other = s + 1 if s % 2 else s - 1
        for t in range(tile):
            here = flat(s, t)
            mates.append((here, flat(mate, t)))
            across.append((here, flat(s, 1 - t)))
            mates_across.append((here, flat(mate, 1 - t)))
            if 0 <= other < scan:
                others.append((here, flat(other, t)))
                others_across.append((here, flat(other, 1 - t)))
    return mates, others, across, mates_across, others_across


def send(array, pairs):
    return lax.ppermute(array, AXES, pairs)


def peers(scan, tile, scan_flip, tile_flip):
    return [
        (s * tile + t, (s ^ scan_flip) * tile + (t ^ tile_flip))
        for s in range(scan)
        for t in range(tile)
    ]


def probe_update(where, probe_chip, keeps, sends, mates, scan, tile):
    modes, _, n, _ = probe_chip.shape
    group = [peers(scan, tile, 2 * (k // 2), k % 2) for k in range(1, 4)]
    smem = pl.BlockSpec(memory_space=pltpu.SMEM)
    joined = []
    for keep, other in zip(keeps, sends):
        planes, rows, _ = keep.shape
        received = send(other, mates)
        block = pltpu.VMEM((planes, rows // 4, n), f32)
        own, *others = pl.pallas_call(
            split_kernel,
            out_shape=(block,) * 4,
            in_specs=[smem] + vmem(2),
            out_specs=tuple(vmem(4)),
            name="split",
        compiler_params=limit(4),
        )(where, *on_chip(keep, received))
        total = own
        arrived = [send(other, perm) for other, perm in zip(others, group)]
        total = own + arrived[0] + arrived[1] + arrived[2]
        flip = 4
        while flip < scan:
            total = total + send(total, peers(scan, tile, 2 * flip - 4, 0))
            flip = flip * 2
        arrived = [send(total, perm) for perm in group]
        mine = pl.pallas_call(
            join_kernel,
            out_shape=pltpu.VMEM(keep.shape, f32),
            in_specs=[smem] + vmem(4),
            out_specs=vmem(1)[0],
            name="join",
        compiler_params=limit(4),
        )(where, *on_chip(total, *arrived))
        joined += [mine, send(mine, mates)]
    planes = 2 * modes
    return pl.pallas_call(
        probe_kernel,
        out_shape=jax.ShapeDtypeStruct((planes, n, n), f32),
        in_specs=[smem] + vmem(1 + 2 * PARTS),
        out_specs=pl.BlockSpec(memory_space=pl.ANY),
        scratch_shapes=[
            pltpu.VMEM((-(-planes // 32) * 32, n, n), f32),
            pltpu.VMEM((planes + 2, n, n), f32),
            pltpu.VMEM((planes, n, n), f32),
            pltpu.VMEM((8 * planes, 8 * planes), f32),
            pltpu.SemaphoreType.DMA((n // 32,)),
        ],
        name="probe",
        compiler_params=limit(20),
    )(where, *on_chip(probe_chip, *joined))


def program(probe_modes, patterns, specimen, offsets):
    modes, _, n, _ = probe_modes.shape
    count = patterns.shape[0]
    rows, cols = specimen.shape[1:]
    scan = lax.axis_size("scan")
    tile = lax.axis_size("tile")
    assert tile == 2 and scan >= 4 and scan & (scan - 1) == 0 and rows == n and modes % 2 == 0
    s = lax.axis_index("scan")
    t = lax.axis_index("tile")
    where = jnp.concatenate(
        [
            offsets[:, 0] - (s * rows - n),
            offsets[:, 1] - (t * cols - n),
            jnp.stack([s % 2, t, s // 2 % 2 * 2 + t]).astype(jnp.int32),
        ]
    )
    pairs = partners(scan, tile)
    strip = lax.dynamic_slice(specimen, (0, 0, (1 - t) * (cols - n)), (2, rows, n))
    side_b = send(specimen, pairs[1])
    strip_b = send(strip, pairs[4])
    strip_y = send(strip, pairs[2])
    strip_a = send(strip, pairs[3])
    side_a = send(specimen, pairs[0])

    inputs = (probe_modes, patterns, specimen, *dft_tables(n))
    probe_chip, _, own, *tables, power, root, measured = pl.pallas_call(
        prepare_kernel,
        out_shape=tuple(pltpu.VMEM(a.shape, a.dtype) for a in inputs)
        + (
            pltpu.VMEM((n, n), f32), pltpu.VMEM((count, n, n), f32), pltpu.VMEM((8, n), f32),
        ),
        in_specs=[pl.BlockSpec(memory_space=pltpu.HBM)] * 7,
        out_specs=tuple(vmem(10)),
        scratch_shapes=[pltpu.SemaphoreType.DMA((7,))],
        name="prepare",
        compiler_params=limit(8),
    )(*(pltpu.with_memory_space_constraint(a, pltpu.HBM) for a in inputs))

    wide = pltpu.VMEM((3, rows, cols), f32)
    column = pltpu.VMEM((3, 3, rows, n), f32)
    planes = 2 * modes + 2
    ext_rows = rows + 2 * n + 8
    ext_cols = cols + 3 * n
    part = pltpu.VMEM((planes // PARTS, n // 2, n), f32)
    *halves, fold_own, fold_a, fold_b, fold_y = pl.pallas_call(
        positions_kernel,
        out_shape=(part,) * (2 * PARTS) + (wide, wide, wide, column),
        in_specs=[pl.BlockSpec(memory_space=pltpu.SMEM)] + vmem(14),
        out_specs=tuple(vmem(4 + 2 * PARTS)),
        scratch_shapes=[
            pltpu.VMEM((planes, n, n), f32),
            pltpu.VMEM((2, ext_rows, ext_cols), f32),
            pltpu.VMEM((3, ext_rows, ext_cols), f32),
            pltpu.VMEM((modes // 2, 2 * n, 2 * n), f32),
            pltpu.VMEM((2, n, n), f32),
            pltpu.VMEM((n, n), f32),
            pltpu.VMEM((2, n, n), f32),
        ],
        name="positions",
        compiler_params=limit(30),
    )(
        where,
        *on_chip(
            probe_chip, root, power, measured, own, side_a, side_b, strip_y, strip_a, strip_b,
            *tables,
        ),
    )

    keeps, sends = halves[0::2], halves[1::2]
    back_y = send(fold_y, pairs[2])
    fold_own, fold_a, fold_b = pl.pallas_call(
        edge_kernel,
        out_shape=(wide,) * 3,
        in_specs=[pl.BlockSpec(memory_space=pltpu.SMEM)] + vmem(4),
        out_specs=tuple(vmem(3)),
        name="edges",
        compiler_params=limit(6),
    )(where, *on_chip(back_y, fold_own, fold_a, fold_b))
    back_b = send(fold_b, pairs[1])
    back_a = send(fold_a, pairs[0])

    new_probe = probe_update(where, probe_chip, keeps, sends, pairs[0], scan, tile)
    new_specimen = finish(new_probe, own, fold_own, back_a, back_b)
    return (new_probe.reshape(probe_modes.shape), new_specimen)


def finish(after, own, *folds):
    return pl.pallas_call(
        object_kernel,
        out_shape=jax.ShapeDtypeStruct(own.shape, f32),
        in_specs=vmem(4) + [pl.BlockSpec(memory_space=pltpu.HBM)],
        out_specs=vmem(1)[0],
        name="object",
        compiler_params=limit(4),
    )(*on_chip(own, *folds), pltpu.with_memory_space_constraint(after, pltpu.HBM))


def solution(mesh):
    return jax.shard_map(
        program,
        mesh=mesh,
        in_specs=(
            P(),
            P(AXES, None, None),
            P(None, "scan", "tile"),
            P(AXES, None),
        ),
        out_specs=(P(), P(None, "scan", "tile")),
        check_vma=False,
    )
```
